768 devices in a mesh: blk: 16 (over x_lo, y), fsdp: 48 (over z, x_hi, core).
Axes of the slice: x: 4 (x_hi: 2, x_lo: 2; x = x_hi * 2 + x_lo), y: 8, z: 12, core: 2. Of those that a mesh axis runs over, the one named last changes fastest.
Arguments:
- tokens: bfloat16 [16, 6144, 2304], P('blk', 'fsdp'), may hold values from -6 to 6
- cotangent: bfloat16 [16, 6144, 512], P('blk', 'fsdp'), may hold values from -6 to 6
- weights: float32 [16, 2304, 512], P('blk', 'fsdp'), may hold values from -6 to 6
- moment_one: float32 [16, 2304, 512], P('blk', 'fsdp'), may hold values from -6 to 6
- moment_two: float32 [16, 2304, 512], P('blk', 'fsdp'), may hold values from 1 to 16
- gossip: int32 [16, 3], P('blk'), may hold values from 1 to 8
Outputs:
- key_out: bfloat16 [16, 6144, 512], P('blk', 'fsdp')
- input_grad: bfloat16 [16, 6144, 2304], P('blk', 'fsdp')
- weights_out: float32 [16, 2304, 512], P('blk', 'fsdp')
- moment_one_out: float32 [16, 2304, 512], P('blk', 'fsdp')
- moment_two_out: float32 [16, 2304, 512], P('blk', 'fsdp')
The draws below stay inside these ranges and needn't reach their ends.
Inputs may be any that keep to these rules, and one draw needn't show every extreme that they name: `gossip`: row r holds the weights given to replica r - 1, to replica r itself and to replica r + 1 on the closed cycle of 16 replicas.
All inputs are finite; a program needn't handle non-finite values.
Results may differ from the reference program's by a relative error of at most 0.005.
Values may be sent and summed in bfloat16 or wider, within the bound.
No kernel may reach another device: no remote copies, remote signals or barrier semaphores. Data moves between devices by JAX's collectives and lax.ppermute only.
A program may use at most 32 MiB of HBM per device.

```python
import math
import jax
import jax.numpy as jnp
from jax import lax

DIN = 2304
HKD = 512
TOKENS = 6144
REPLICAS = 16


def touch_ends(result, stream_key, smallest, top_value):
    longest = result.shape.index(max(result.shape))
    spots = []
    for shift in (0, 1):
        where = [jax.random.randint(jax.random.fold_in(stream_key, axis), (), 0, length) for axis, length in enumerate(result.shape)]
        where[longest] = (where[longest] + shift) % result.shape[longest]
        spots.append(tuple(where))
    return result.at[spots[0]].set(smallest).at[spots[1]].set(top_value)


def raised(values, own_key, source, target, blocks, factor):
    def block_of(dim):
        return (jnp.arange(values.shape[dim]) // (values.shape[dim] // blocks)).reshape((-1,) + (1,) * (values.ndim - 1 - dim))

    one_side = jax.random.permutation(own_key, blocks)[block_of(target)]
    second = (block_of(target) + blocks // 2) % blocks
    return jnp.where((block_of(source) == one_side) | (block_of(source) == second), factor * values, values)


def levels(stream_key, extent, cuts, smallest, high):
    loudness, own = 1.0, jax.random.fold_in(stream_key, 6)
    for dim, blocks in cuts:
        heights = jnp.exp(jax.random.uniform(jax.random.fold_in(own, dim), (blocks,), jnp.float32, smallest / len(cuts), high / len(cuts)))
        loudness = loudness * jnp.repeat(heights, extent[dim] // blocks).reshape([-1 if axis == dim else 1 for axis in range(len(extent))])
    return loudness


def scatter_about(rng, extent, scale, most, split=(), dtype=jnp.bfloat16):
    values = scale * jax.random.normal(rng, extent, jnp.float32)
    if split:
        values = values * levels(rng, extent, split, -0.22, 0.18)
    return jnp.clip(values, -most, most).astype(dtype)


def bell_draw_with(key, shape, spread, most, shards, heavy, held_as=jnp.bfloat16):
    drawn = spread * jax.random.normal(key, shape, jnp.float32)
    if shards:
        drawn = drawn * levels(key, shape, shards, -0.22, 0.18)
    return jnp.clip(raised(drawn, jax.random.fold_in(key, 3), *heavy), -most, most).astype(held_as)


def setup_inputs(seed: int = 0) -> dict:
    keys = jax.random.split(jax.random.key(seed), 7)
    tokens = bell_draw_with(keys[0], (REPLICAS, TOKENS, DIN), 1.0, 6.0, ((0, 16), (1, 48)), (1, 2, 48, 3.25))
    cotangent = scatter_about(keys[1], (REPLICAS, TOKENS, HKD), 1.0, 6.0, ((0, 16), (1, 48)))
    weights = scatter_about(keys[2], (REPLICAS, DIN, HKD), 1.0, 6.0, ((0, 16), (1, 48)), jnp.float32)
    moment_one = scatter_about(keys[3], (REPLICAS, DIN, HKD), 1.0, 6.0, ((0, 16), (1, 48)), jnp.float32)
    moment_two = jnp.clip(jnp.exp(math.log(16.0) - 2.7725887 * jax.random.uniform(keys[4], (REPLICAS, DIN, HKD), jnp.float32) ** levels(keys[4], (REPLICAS, DIN, HKD), ((0, 16), (1, 48)), -0.2, 0.2)), 1.0, 16.0)
    gossip = touch_ends(jax.random.randint(keys[5], (REPLICAS, 3), 1, 9), jax.random.fold_in(keys[5], 1), 1, 8).astype(jnp.int32)
    return {"tokens": tokens, "cotangent": cotangent, "weights": weights, "moment_one": moment_one, "moment_two": moment_two, "gossip": gossip}


beta_one = 0.9
beta_two = 0.95
learn_rate = 0.05
weight_decay = 0.1
epsilon = 1e-08
correct_one = 1.0 - beta_one ** 5
correct_two = 1.0 - beta_two ** 5

def replica_step(inputs):
    activations, upstream, weights, moment_one, moment_two = inputs
    factor = 1.0 / math.sqrt(DIN)
    compute_weights = weights.astype(jnp.bfloat16)
    key_out = (jnp.dot(activations, compute_weights, preferred_element_type=jnp.float32) * factor).astype(jnp.bfloat16)
    input_grad = (jnp.dot(upstream, compute_weights.T, preferred_element_type=jnp.float32) * factor).astype(jnp.bfloat16)
    gradient = jnp.dot(activations.T, upstream, preferred_element_type=jnp.float32) * factor
    moment_one_out = beta_one * moment_one + (1.0 - beta_one) * gradient
    moment_two_out = beta_two * moment_two + (1.0 - beta_two) * gradient * gradient
    update = moment_one_out / correct_one / (jnp.sqrt(moment_two_out / correct_two) + epsilon)
    stepped = weights - learn_rate * (update + weight_decay * weights)
    return (key_out, input_grad, stepped, moment_one_out, moment_two_out)

def reference(tokens, cotangent, weights, moment_one, moment_two, gossip):
    key_out, input_grad, stepped, moment_one_out, moment_two_out = lax.map(replica_step, (tokens, cotangent, weights, moment_one, moment_two))
    left_side = jnp.roll(stepped, 1, axis=0)
    right_side = jnp.roll(stepped, -1, axis=0)
    mix_weights = gossip.astype(jnp.float32)
    weight_left = mix_weights[:, 0][:, None, None]
    weight_self = mix_weights[:, 1][:, None, None]
    weight_right = mix_weights[:, 2][:, None, None]
    weights_out = (weight_left * left_side + weight_self * stepped + weight_right * right_side) / (weight_left + weight_self + weight_right)
    return (key_out, input_grad, weights_out, moment_one_out, moment_two_out)
```

```python
import functools
import math

import jax
import jax.numpy as jnp
from jax import lax
from jax.experimental import pallas as pl
from jax.experimental.pallas import tpu as pltpu
from jax.sharding import Mesh
from jax.sharding import PartitionSpec as P

FSDP = ("z", "xh", "core")


beta_one = 0.9
beta_two = 0.95
learn_rate = 0.05
weight_decay = 0.1
epsilon = 1e-08
correct_one = 1.0 - beta_one**5
correct_two = 1.0 - beta_two**5

f32, bf16 = jnp.float32, jnp.bfloat16


def swap(shard, axis):
    return lax.ppermute(shard, axis, [(0, 1), (1, 0)])


def from_behind(shard, axis, by):
    length = lax.axis_size(axis)
    return lax.ppermute(shard, axis, [(i, (i + by) % length) for i in range(length)])


def kernel_call(body, ins, outs, flops, scratch=()):
    vmem, smem = pltpu.VMEM, pltpu.SMEM
    moved = sum(a.size * a.dtype.itemsize for a in (*ins, *outs))
    limit = moved + sum(math.prod(s.shape) * 2 for s in scratch) + (4 << 20)
    return pl.pallas_call(
        body,
        out_shape=outs,
        in_specs=[pl.BlockSpec(memory_space=smem if a.size < 8 else vmem) for a in ins],
        out_specs=[pl.BlockSpec(memory_space=vmem) for _ in outs],
        scratch_shapes=scratch,
        compiler_params=pltpu.CompilerParams(vmem_limit_bytes=limit),
        cost_estimate=pl.CostEstimate(flops=flops, bytes_accessed=moved, transcendentals=0),
    )(*ins)


def choose(flag, first, second):
    return jnp.where(flag == 0, first, second), jnp.where(flag == 0, second, first)


def terms_body(factor, place, activations, upstream, keep, give):
    chunk = 384
    pairs = chunk // (2 * 48)
    right = upstream[...]
    for i in range(activations.shape[1] // chunk):
        left = activations[:, i * chunk : (i + 1) * chunk]
        part = lax.dot_general(left, right, (((0,), (0,)), ((), ())), preferred_element_type=f32)
        part = (part * factor).reshape(pairs, 2, 48, right.shape[1])
        mine, theirs = choose(place[1], part[:, 0], part[:, 1])
        keep[i * pairs : (i + 1) * pairs] = mine
        give[i * pairs : (i + 1) * pairs] = theirs.astype(bf16)


def core_sum_body(place, keep, theirs, keep_x, give_x):
    for z in range(keep_x.shape[0]):
        low, high = (keep[2 * z + k] + theirs[2 * z + k].astype(f32) for k in (0, 1))
        mine, other = choose(place[0], low, high)
        keep_x[z] = mine
        give_x[z] = other.astype(bf16)


def x_sum_body(keep, theirs, terms):
    for z in range(keep.shape[0]):
        terms[z] = (keep[z] + theirs[z].astype(f32)).astype(bf16)


def adam_body(terms, master, one, two, one_out, two_out, stepped, stepped_low):
    for row in range(0, master.shape[0], 16):
        rows = slice(row, row + 16)
        gradient = terms[0, rows].astype(f32)
        for z in range(1, terms.shape[0]):
            gradient = gradient + terms[z, rows].astype(f32)
        first = beta_one * one[rows] + (1.0 - beta_one) * gradient
        second = beta_two * two[rows] + (1.0 - beta_two) * gradient * gradient
        one_out[rows] = first
        two_out[rows] = second
        update = first / correct_one / (jnp.sqrt(second / correct_two) + epsilon)
        value = master[rows] - learn_rate * (update + weight_decay * master[rows])
        stepped[rows] = value
        stepped_low[rows] = value.astype(bf16)


def use_body(factor, place, own, x, core, core_x, activations, upstream, key_out, input_grad, full):
    rows = own.shape[1]
    for piece, xh, c in (
        (own, place[0], place[1]),
        (x, 1 - place[0], place[1]),
        (core, place[0], 1 - place[1]),
        (core_x, 1 - place[0], 1 - place[1]),
    ):
        for z in range(own.shape[0]):
            start = pl.multiple_of(z * 4 * rows + (2 * xh + c) * rows, 16)
            full[pl.ds(start, rows), :] = piece[z]
    left = upstream[...]
    chunk = 256
    for i in range(full.shape[0] // chunk):
        part = lax.dot_general(
            left,
            full[i * chunk : (i + 1) * chunk, :],
            (((1,), (1,)), ((), ())),
            preferred_element_type=f32,
        )
        input_grad[:, i * chunk : (i + 1) * chunk] = (part * factor).astype(bf16)
    part = jnp.dot(activations[...], full[...], preferred_element_type=f32)
    key_out[...] = (part * factor).astype(bf16)


def local(tokens, cotangent, weights, moment_one, moment_two, gossip):
    activations = tokens[0]
    upstream = cotangent[0]
    factor = 1.0 / math.sqrt(activations.shape[1])
    place = jnp.stack([lax.axis_index("xh"), lax.axis_index("core")]).astype(jnp.int32)
    length = lax.axis_size("z")
    rows, keys = weights.shape[1:]
    flops = 2 * activations.size * keys
    block = lambda lead, dtype: jax.ShapeDtypeStruct((lead, rows, keys), dtype)
    flat = lambda dtype: jax.ShapeDtypeStruct((rows, keys), dtype)

    keep, give = kernel_call(
        functools.partial(terms_body, factor),
        (place, activations, upstream),
        (block(2 * length, f32), block(2 * length, bf16)),
        flops,
    )
    theirs = swap(give, "core")
    keep, give = kernel_call(
        core_sum_body, (place, keep, theirs), (block(length, f32), block(length, bf16)), keep.size
    )
    theirs = swap(give, "xh")

    compute_weights = weights[0].astype(bf16)
    column = lax.all_gather(compute_weights, "z", axis=0)
    column_x = swap(column, "xh")
    column_core = swap(column, "core")

    (terms,) = kernel_call(x_sum_body, (keep, theirs), (block(length, bf16),), keep.size)
    terms = lax.all_to_all(terms, "z", 0, 0, tiled=True)

    moment_one_out, moment_two_out, stepped, stepped_low = kernel_call(
        adam_body,
        (terms, weights[0], moment_one[0], moment_two[0]),
        (flat(f32), flat(f32), flat(f32), flat(bf16)),
        terms.size,
    )
    left_side = from_behind(stepped_low, "blk", 1).astype(f32)
    right_side = from_behind(stepped_low, "blk", -1).astype(f32)
    mix_weights = gossip[0].astype(f32)
    averaged = (
        mix_weights[0] * left_side + mix_weights[1] * stepped + mix_weights[2] * right_side
    ) / (mix_weights[0] + mix_weights[1] + mix_weights[2])

    column_core_x = swap(column_x, "core")
    key_out, input_grad = kernel_call(
        functools.partial(use_body, factor),
        (place, column, column_x, column_core, column_core_x, activations, upstream),
        (
            jax.ShapeDtypeStruct((activations.shape[0], keys), bf16),
            jax.ShapeDtypeStruct(activations.shape, bf16),
        ),
        2 * flops,
        (pltpu.VMEM((4 * length * rows, keys), bf16),),
    )
    return (
        key_out[None],
        input_grad[None],
        averaged[None],
        moment_one_out[None],
        moment_two_out[None],
    )


def solution(mesh):
    split = Mesh(mesh.devices.reshape(mesh.shape["blk"], 12, 2, 2), ("blk",) + FSDP)
    spec = P("blk", FSDP, None)

    return jax.shard_map(
        local,
        mesh=split,
        in_specs=(spec,) * 5 + (P("blk", None),),
        out_specs=(spec,) * 5,
        check_vma=False,
    )
```

```python
import functools
import math

import jax
import jax.numpy as jnp
from jax import lax
from jax.experimental import pallas as pl
from jax.experimental.pallas import tpu as pltpu
from jax.sharding import Mesh
from jax.sharding import PartitionSpec as P

FSDP = ("z", "xh", "core")


beta_one = 0.9
beta_two = 0.95
learn_rate = 0.05
weight_decay = 0.1
epsilon = 1e-08
correct_one = 1.0 - beta_one**5
correct_two = 1.0 - beta_two**5

f32, bf16 = jnp.float32, jnp.bfloat16


def swap(shard, axis):
    return lax.ppermute(shard, axis, [(0, 1), (1, 0)])


def from_behind(shard, axis, by):
    length = lax.axis_size(axis)
    return lax.ppermute(shard, axis, [(i, (i + by) % length) for i in range(length)])


def kernel_call(body, ins, outs, flops, scratch=()):
    vmem, smem = pltpu.VMEM, pltpu.SMEM
    moved = sum(a.size * a.dtype.itemsize for a in (*ins, *outs))
    limit = moved + sum(math.prod(s.shape) * 2 for s in scratch) + (4 << 20)
    return pl.pallas_call(
        body,
        out_shape=outs,
        in_specs=[pl.BlockSpec(memory_space=smem if a.size < 8 else vmem) for a in ins],
        out_specs=[pl.BlockSpec(memory_space=vmem) for _ in outs],
        scratch_shapes=scratch,
        compiler_params=pltpu.CompilerParams(vmem_limit_bytes=limit),
        cost_estimate=pl.CostEstimate(flops=flops, bytes_accessed=moved, transcendentals=0),
    )(*ins)


def choose(flag, first, second):
    return jnp.where(flag == 0, first, second), jnp.where(flag == 0, second, first)


def terms_body(factor, place, activations, upstream, keep, give):
    chunk = 384
    pairs = chunk // (2 * 48)
    right = upstream[...]
    for i in range(activations.shape[1] // chunk):
        left = activations[:, i * chunk : (i + 1) * chunk]
        part = lax.dot_general(left, right, (((0,), (0,)), ((), ())), preferred_element_type=f32)
        part = (part * factor).reshape(pairs, 2, 48, right.shape[1])
        mine, theirs = choose(place[1], part[:, 0], part[:, 1])
        keep[i * pairs : (i + 1) * pairs] = mine
        give[i * pairs : (i + 1) * pairs] = theirs.astype(bf16)


def core_sum_body(place, keep, theirs, keep_x, give_x):
    for z in range(keep_x.shape[0]):
        low, high = (keep[2 * z + k] + theirs[2 * z + k].astype(f32) for k in (0, 1))
        mine, other = choose(place[0], low, high)
        keep_x[z] = mine
        give_x[z] = other.astype(bf16)


def x_sum_body(keep, theirs, terms):
    for z in range(keep.shape[0]):
        terms[z] = (keep[z] + theirs[z].astype(f32)).astype(bf16)


def adam_body(terms, master, one, two, one_out, two_out, stepped, stepped_low):
    for row in range(0, master.shape[0], 16):
        rows = slice(row, row + 16)
        gradient = terms[0, rows].astype(f32)
        for z in range(1, terms.shape[0]):
            gradient = gradient + terms[z, rows].astype(f32)
        first = beta_one * one[rows] + (1.0 - beta_one) * gradient
        second = beta_two * two[rows] + (1.0 - beta_two) * gradient * gradient
        one_out[rows] = first
        two_out[rows] = second
        update = first / correct_one / (jnp.sqrt(second / correct_two) + epsilon)
        value = master[rows] - learn_rate * (update + weight_decay * master[rows])
        stepped[rows] = value
        stepped_low[rows] = value.astype(bf16)


def use_body(factor, place, own, x, core, core_x, activations, upstream, key_out, input_grad, full):
    rows = own.shape[1]
    for piece, xh, c in (
        (own, place[0], place[1]),
        (x, 1 - place[0], place[1]),
        (core, place[0], 1 - place[1]),
        (core_x, 1 - place[0], 1 - place[1]),
    ):
        for z in range(own.shape[0]):
            start = pl.multiple_of((4 * z + 2 * xh + c) * rows, 16)
            full[pl.ds(start, rows), :] = piece[z]
    left = upstream[...]
    chunk = 256
    for i in range(full.shape[0] // chunk):
        part = lax.dot_general(
            left,
            full[i * chunk : (i + 1) * chunk, :],
            (((1,), (1,)), ((), ())),
            preferred_element_type=f32,
        )
        input_grad[:, i * chunk : (i + 1) * chunk] = (part * factor).astype(bf16)
    part = jnp.dot(activations[...], full[...], preferred_element_type=f32)
    key_out[...] = (part * factor).astype(bf16)


def mix_body(gossip, left, own, right, out):
    before, self_, after = (gossip[0, k].astype(f32) for k in range(3))
    total = before + self_ + after
    value = before * left[...].astype(f32) + self_ * own[...] + after * right[...].astype(f32)
    out[...] = value / total


def local(tokens, cotangent, weights, moment_one, moment_two, gossip):
    activations = tokens[0]
    upstream = cotangent[0]
    factor = 1.0 / math.sqrt(activations.shape[1])
    place = jnp.stack([lax.axis_index(a) for a in ("xh", "core")]).astype(jnp.int32)
    length = lax.axis_size("z")
    rows, keys = weights.shape[1:]
    flops = 2 * activations.size * keys
    block = lambda lead, dtype: jax.ShapeDtypeStruct((lead, rows, keys), dtype)
    flat = lambda dtype: jax.ShapeDtypeStruct((rows, keys), dtype)

    keep, give = kernel_call(
        functools.partial(terms_body, factor),
        (place, activations, upstream),
        (block(2 * length, f32), block(2 * length, bf16)),
        flops,
    )
    theirs = swap(give, "core")
    keep, give = kernel_call(
        core_sum_body, (place, keep, theirs), (block(length, f32), block(length, bf16)), keep.size
    )
    theirs = swap(give, "xh")

    compute_weights = weights[0].astype(bf16)
    column = lax.all_gather(compute_weights, "z", axis=0)
    column_x = swap(column, "xh")
    column_core = swap(column, "core")

    (terms,) = kernel_call(x_sum_body, (keep, theirs), (block(length, bf16),), keep.size)
    terms = lax.all_to_all(terms, "z", 0, 0, tiled=True)

    moment_one_out, moment_two_out, stepped, stepped_low = kernel_call(
        adam_body,
        (terms, weights[0], moment_one[0], moment_two[0]),
        (flat(f32), flat(f32), flat(f32), flat(bf16)),
        terms.size,
    )
    left_side = from_behind(stepped_low, "blk", 1)
    right_side = from_behind(stepped_low, "blk", -1)
    (averaged,) = kernel_call(
        mix_body, (gossip, left_side, stepped, right_side), (flat(f32),), 5 * stepped.size
    )

    column_core_x = swap(column_x, "core")
    key_out, input_grad = kernel_call(
        functools.partial(use_body, factor),
        (place, column, column_x, column_core, column_core_x, activations, upstream),
        (
            jax.ShapeDtypeStruct((activations.shape[0], keys), bf16),
            jax.ShapeDtypeStruct(activations.shape, bf16),
        ),
        2 * flops,
        (pltpu.VMEM((4 * length * rows, keys), bf16),),
    )
    return (
        key_out[None],
        input_grad[None],
        averaged[None],
        moment_one_out[None],
        moment_two_out[None],
    )


def solution(mesh):
    split = Mesh(mesh.devices.reshape(mesh.shape["blk"], 12, 2, 2), ("blk",) + FSDP)
    spec = P("blk", FSDP, None)

    return jax.shard_map(
        local,
        mesh=split,
        in_specs=(spec,) * 5 + (P("blk", None),),
        out_specs=(spec,) * 5,
        check_vma=False,
    )
```
